32 devices in a mesh: dp: 8 (over z, core), mp: 4 (over y, x).
Axes of the slice: x: 2, y: 2, z: 4, core: 2. Of those that a mesh axis runs over, the one named last changes fastest.
Arguments:
- master: float32 [4096, 5120], P('dp', 'mp'), may hold values from -60 to 60
- moment_first: float32 [4096, 5120], P('dp', 'mp'), may hold values from -0.06 to 0.06
- moment_second: float32 [4096, 5120], P('dp', 'mp'), may hold values from 1e-05 to 0.001
- gradients: float32 [4096, 5120], P('dp', 'mp'), may hold values from -0.2 to 0.2
- step_count: int32 [1], replicated, may hold values from 1 to 10
- tensor_rows: int32 [24], replicated, may hold values from 1 to 1024, 4096 in all
- decay_mask: int32 [24], replicated, may hold values 0 or 1
Outputs:
- new_master: float32 [4096, 5120], P('dp', 'mp')
- new_first: float32 [4096, 5120], P('dp', 'mp')
- new_second: float32 [4096, 5120], P('dp', 'mp')
- compute_weights: bfloat16 [4096, 5120], P(None, 'mp')
The draws below stay inside these ranges and needn't reach their ends.
Inputs may be any that keep to these rules, and one draw needn't show every extreme that they name: `tensor_rows`: the rows sum to 4096; the largest tensor has 1024 rows.
All inputs are finite; a program needn't handle non-finite values.
Results may differ from the reference program's by a relative error of at most 0.0004.
Values may be sent and summed in bfloat16 or wider, within the bound.
A program may use at most 128 MiB of HBM per device.

```python
import math
import jax
import jax.numpy as jnp
import numpy as np
from jax import lax

WIDE = 5120
TENSORS = 24
ROWS = 4096
MOST = 1024


def draw_master(key, part):
    keys = jax.random.split(key, 3)
    row_scale = jnp.exp(jax.random.uniform(keys[0], (ROWS, 1), jnp.float32, -1.2, 1.2))
    col_scale = jnp.exp(jax.random.uniform(keys[1], (1, WIDE), jnp.float32, -1.2, 1.2))
    ramp = 1.0 + 2.0 * jnp.arange(ROWS, dtype=jnp.float32)[:, None] / ROWS
    base = jax.random.normal(keys[2], (ROWS, WIDE), jnp.float32)
    values = 0.3 * base * row_scale * col_scale * ramp
    return jnp.clip(values, -60.0, 60.0).astype(jnp.float32)


def set_ends(entries, key, low, top_value):
    longest = entries.shape.index(max(entries.shape))
    spots = []
    for shift in (0, 1):
        where = [jax.random.randint(jax.random.fold_in(key, axis), (), 0, length) for axis, length in enumerate(entries.shape)]
        where[longest] = (where[longest] + shift) % entries.shape[longest]
        spots.append(tuple(where))
    return entries.at[spots[0]].set(low).at[spots[1]].set(top_value)


def block_levels(own_key, dims, shards, low, high):
    level = 1.0
    for axis_at, shards_of in shards:
        draws = jax.random.uniform(jax.random.fold_in(jax.random.fold_in(own_key, 6), axis_at), (shards_of,), jnp.float32, low / len(shards), high / len(shards))
        level = level * jnp.repeat(jnp.exp(draws), dims[axis_at] // shards_of).reshape((-1,) + (1,) * (len(dims) - 1 - axis_at))
    return level


def profile(count, total, limit, slope):
    loads = [(1 << 20) // math.isqrt(grade ** slope) + 1 for grade in range(2, count + 1)]
    rest, counts = total - limit - (count - 1), [1] * (count - 1)
    while rest > 0:
        movable = [i for i in range(count - 1) if counts[i] < limit]
        pool, budget = sum([loads[i] for i in movable]), rest
        for i in movable:
            more = min(limit - counts[i], max(1, budget * loads[i] // pool), rest)
            counts[i] = counts[i] + more
            rest = rest - more
    return np.array([limit] + counts)


def ragged_sizes(stream_key, amount, total, most, slope):
    if amount == 2:
        one = jax.random.randint(stream_key, (), max(1, total - most), min(most, total - 1) + 1)
        return jnp.stack([one, total - one])
    tallies = jnp.asarray(profile(amount, total, most, slope), jnp.int32)
    pairs = (amount - 1) // 2
    source_of, taker = tallies[1:1 + 2 * pairs:2], tallies[2:2 + 2 * pairs:2]
    room = jnp.minimum(source_of - 1, most - taker)
    shifted = jax.random.randint(jax.random.fold_in(stream_key, 1), (pairs,), 0, 1 << 20) % (room + 1)
    tallies = tallies.at[1:1 + 2 * pairs:2].set(source_of - shifted).at[2:2 + 2 * pairs:2].set(taker + shifted)
    return tallies[jax.random.permutation(jax.random.fold_in(stream_key, 2), amount)]


def bell_draw(key, dims, width, bound, cuts=(), held_as=jnp.bfloat16):
    gain = block_levels(key, dims, cuts, -0.22, 0.18) if cuts else 1.0
    values = jax.random.normal(key, dims, jnp.float32) * width * gain
    return jnp.minimum(jnp.maximum(values, -bound), bound).astype(held_as)


def setup_inputs(seed: int = 0) -> dict:
    arg_keys = jax.random.split(jax.random.key(seed), 8)
    master = draw_master(jax.random.fold_in(arg_keys[7], 71), 0)
    moment_first = bell_draw(arg_keys[1], (ROWS, WIDE), 0.01, 0.06, ((0, 8), (1, 4)), jnp.float32)
    moment_second = jnp.clip(jnp.exp(math.log(0.001) - 4.6051703 * jax.random.uniform(arg_keys[2], (ROWS, WIDE), jnp.float32) ** block_levels(arg_keys[2], (ROWS, WIDE), ((0, 8), (1, 4)), -0.2, 0.2)), 9.999999747378752e-06, 0.001)
    gradients = bell_draw(arg_keys[3], (ROWS, WIDE), 0.03, 0.2, ((0, 8), (1, 4)), jnp.float32)
    step_count = jax.random.randint(arg_keys[4], (1,), 1, 11).astype(jnp.int32)
    tensor_rows = ragged_sizes(arg_keys[5], TENSORS, ROWS, MOST, 1).astype(jnp.int32)
    decay_mask = set_ends((jax.random.randint(arg_keys[6], (TENSORS,), 0, 2) < 1).astype(jnp.int32), jax.random.fold_in(arg_keys[6], 1), 0, 1)
    return dict(master=master, moment_first=moment_first, moment_second=moment_second, gradients=gradients, step_count=step_count, tensor_rows=tensor_rows, decay_mask=decay_mask)


beta_first = 0.9
beta_second = 0.999
adam_epsilon = 1e-06
decay_rate = 0.3
learn_rate = 0.3
norm_epsilon = 1e-06

def reference(master, moment_first, moment_second, gradients, step_count, tensor_rows, decay_mask):
    steps = step_count[0].astype(jnp.float32)
    new_first = beta_first * moment_first + (1.0 - beta_first) * gradients
    new_second = beta_second * moment_second + (1.0 - beta_second) * gradients * gradients
    fix_first = 1.0 - jnp.power(jnp.float32(beta_first), steps)
    fix_second = 1.0 - jnp.power(jnp.float32(beta_second), steps)
    offsets = (jnp.cumsum(tensor_rows) - tensor_rows).astype(jnp.int32)
    row_ids = jnp.arange(ROWS, dtype=jnp.int32)
    segment = (lax.optimization_barrier(jnp.sum((row_ids[:, None] >= offsets[None, :]).astype(jnp.int32), axis=1)) - 1).astype(jnp.int32)
    mask_rows = decay_mask.astype(jnp.float32)[segment]
    update = new_first / fix_first / (jnp.sqrt(new_second / fix_second) + adam_epsilon)
    update = update + decay_rate * mask_rows[:, None] * master
    weight_sq = jax.ops.segment_sum(lax.optimization_barrier(jnp.sum(master * master, axis=1)), segment, num_segments=TENSORS)
    update_sq = jax.ops.segment_sum(lax.optimization_barrier(jnp.sum(update * update, axis=1)), segment, num_segments=TENSORS)
    ratio = jnp.sqrt(weight_sq) / (jnp.sqrt(update_sq) + norm_epsilon)
    new_master = master - learn_rate * ratio[segment][:, None] * update
    return (new_master, new_first, new_second, new_master.astype(jnp.bfloat16))
```

```python
import functools

import jax
import jax.numpy as jnp
from jax import lax
from jax.experimental import pallas as pl
from jax.experimental.pallas import tpu as pltpu
from jax.sharding import PartitionSpec as P

MESH = pl.DeviceIdType.MESH

beta_first = 0.9
beta_second = 0.999
adam_epsilon = 1e-06
decay_rate = 0.3
learn_rate = 0.3
norm_epsilon = 1e-06

LOADS = 8
CHUNKS = 4
GROUP = 16
HALF = 64


def power(base, exponent):
    result = jnp.float32(1.0)
    factor = jnp.float32(base)
    for bit in range(31):
        taken = ((exponent >> bit) & 1) == 1
        result = jnp.where(taken, result * factor, result)
        factor = factor * factor
    return result


def kernel(dp, mp, tensors, step_ref, rows_ref, mask_ref, m_hbm, f_hbm, s_hbm, g_hbm,
           nm_ref, nf_ref, ns_ref, x_ref,
           mb, fb, sb, gb, mine, mp_buf, mine2, dp_buf,
           load_sem, mp_send, mp_recv, dp_send, dp_recv,
           up_send, up_recv, down_send, down_recv, sib_send, sib_recv):
    rows, wide = m_hbm.shape
    me = lax.axis_index("dp")
    col = lax.axis_index("mp")
    chips = dp // 2
    chip, core = me // 2, me % 2
    sibling = me + 1 - 2 * core
    piece = rows // LOADS
    part = rows // CHUNKS

    def loads(i):
        at = pl.ds(i * piece, piece)
        pairs = ((m_hbm, mb), (f_hbm, fb), (s_hbm, sb), (g_hbm, gb))
        return [pltpu.make_async_copy(a.at[at], b.at[at], load_sem.at[n, i]) for n, (a, b) in enumerate(pairs)]

    for i in range(LOADS):
        for copy in loads(i):
            copy.start()

    barrier = pltpu.get_barrier_semaphore()
    for d in range(1, mp):
        pl.semaphore_signal(barrier, inc=1, device_id={"mp": lax.rem(col + d, mp)}, device_id_type=MESH)
    for d in range(1, dp):
        pl.semaphore_signal(barrier, inc=1, device_id={"dp": lax.rem(me + d, dp)}, device_id_type=MESH)

    step = step_ref[0]
    fix_first = 1.0 - power(beta_first, step)
    fix_second = 1.0 - power(beta_second, step)
    tile = (8, 128)
    scale = (jnp.full(tile, fix_first, jnp.float32) * lax.rsqrt(jnp.full(tile, fix_second, jnp.float32)))[0, 0]
    shift = fix_first * adam_epsilon

    lane = lax.broadcasted_iota(jnp.int32, (1, 128), 1)
    low = jnp.full((1, 128), -1, jnp.int32)
    high = jnp.full((1, 128), -1, jnp.int32)
    decay = jnp.zeros((1, 128), jnp.float32)
    offset = jnp.int32(0)
    for k in range(tensors):
        here = (lane == k) | (lane == HALF + k)
        after = offset + rows_ref[k]
        low = jnp.where(here, offset, low)
        high = jnp.where(here, after, high)
        decay = jnp.where(lane == k, decay_rate * mask_ref[k].astype(jnp.float32), decay)
        offset = after
    first_half = lane < HALF

    def member(start):
        ids = me * rows + start + lax.broadcasted_iota(jnp.int32, (GROUP, 128), 0)
        return ((ids >= low) & (ids < high)).astype(jnp.float32)

    def stats(i, total):
        at = pl.ds(pl.multiple_of(i * GROUP, GROUP), GROUP)
        inside = member(i * GROUP)
        decay_rows = jnp.sum(inside * decay, axis=1, keepdims=True)
        master, gradient = mb[at], gb[at]
        new_first = beta_first * fb[at] + (1.0 - beta_first) * gradient
        new_second = beta_second * sb[at] + (1.0 - beta_second) * gradient * gradient
        nf_ref[at] = new_first
        ns_ref[at] = new_second
        update = new_first / (scale * jnp.sqrt(new_second) + shift) + decay_rows * master
        gb[at] = update
        weight_sq = jnp.sum(master * master, axis=1, keepdims=True)
        update_sq = jnp.sum(update * update, axis=1, keepdims=True)
        return total + inside * jnp.where(first_half, weight_sq, update_sq)

    total = jnp.zeros((GROUP, 128), jnp.float32)
    steps = piece // GROUP
    for i in range(LOADS):
        for copy in loads(i):
            copy.wait()
        total = lax.fori_loop(i * steps, (i + 1) * steps, stats, total)
    total = jnp.sum(total, axis=0, keepdims=True)

    pl.semaphore_wait(barrier, mp + dp - 2)

    def exchange(axis, count, own, value, source, slots, send, recv):
        source[0] = value
        slots[own] = value
        copies = []
        for d in range(1, count):
            copies.append(pltpu.make_async_remote_copy(
                src_ref=source.at[0], dst_ref=slots.at[own], send_sem=send.at[d], recv_sem=recv.at[d],
                device_id={axis: lax.rem(own + d, count)}, device_id_type=MESH))
        for copy in copies:
            copy.start()
        for copy in copies:
            copy.wait_recv()
        result = slots[0]
        for j in range(1, count):
            result = result + slots[j]
        return result, copies

    total, mp_copies = exchange("mp", mp, col, total, mine, mp_buf, mp_send, mp_recv)
    total, dp_copies = exchange("dp", dp, me, total, mine2, dp_buf, dp_send, dp_recv)
    root = jnp.sqrt(jnp.broadcast_to(total, tile))
    ratio = root / (pltpu.roll(root, HALF, 1) + norm_epsilon)
    ratio = jnp.where(first_half, learn_rate * ratio[0:1], 0.0)

    def block(owner, k):
        return x_ref.at[pl.ds(pl.multiple_of(owner * rows + k * part, part), part)]

    def up(s, k):
        ref = block(me - 2 * s, k)
        return pltpu.make_async_remote_copy(
            src_ref=ref, dst_ref=ref, send_sem=up_send.at[s, k], recv_sem=up_recv.at[s, k],
            device_id={"dp": me + 2}, device_id_type=MESH)

    def down(s, k):
        ref = block(me + 2 * s, k)
        return pltpu.make_async_remote_copy(
            src_ref=ref, dst_ref=ref, send_sem=down_send.at[s, k], recv_sem=down_recv.at[s, k],
            device_id={"dp": me - 2}, device_id_type=MESH)

    def side(j, k):
        ref = block(2 * j + core, k)
        return pltpu.make_async_remote_copy(
            src_ref=ref, dst_ref=ref, send_sem=sib_send.at[j, k], recv_sem=sib_recv.at[j, k],
            device_id={"dp": sibling}, device_id_type=MESH)

    def arrival(recv, s, owner, k, to):
        ref = block(owner, k)
        return pltpu.make_async_remote_copy(
            src_ref=ref, dst_ref=ref, send_sem=up_send.at[0, k], recv_sem=recv.at[s, k],
            device_id={"dp": to}, device_id_type=MESH)

    last = chips - 1

    def final(i, carry):
        at = pl.ds(pl.multiple_of(i * GROUP, GROUP), GROUP)
        rate = jnp.sum(member(i * GROUP) * ratio, axis=1, keepdims=True)
        new_master = mb[at] - rate * gb[at]
        nm_ref[at] = new_master
        x_ref[pl.ds(pl.multiple_of(me * rows + i * GROUP, GROUP), GROUP)] = new_master.astype(jnp.bfloat16)
        return carry

    def send_own(k):
        @pl.when(chip < last)
        def _():
            up(0, k).start()

        @pl.when(chip > 0)
        def _():
            down(0, k).start()

        side(chip, k).start()

    groups = part // GROUP
    for k in range(CHUNKS):
        lax.fori_loop(k * groups, (k + 1) * groups, final, 0)
        if k > 0:
            send_own(k - 1)
    for copy in mp_copies + dp_copies:
        copy.wait_send()
    send_own(CHUNKS - 1)

    for s in range(last):
        for k in range(CHUNKS):
            @pl.when(s < chip)
            def _():
                arrival(up_recv, s, me - 2 * (s + 1), k, sibling).wait_recv()

                @pl.when(chip < last)
                def _():
                    up(s + 1, k).start()

                side(chip - (s + 1), k).start()

            @pl.when(s < last - chip)
            def _():
                arrival(down_recv, s, me + 2 * (s + 1), k, sibling).wait_recv()

                @pl.when(chip > 0)
                def _():
                    down(s + 1, k).start()

                side(chip + (s + 1), k).start()

    for s in range(chips):
        for k in range(CHUNKS):
            if s < last or last == 0:
                @pl.when((chip < last) & (s <= chip))
                def _():
                    up(s, k).wait_send()

                @pl.when((chip > 0) & (s <= last - chip))
                def _():
                    down(s, k).wait_send()

            side(s, k).wait_send()
            arrival(sib_recv, s, 2 * s + 1 - core, k, sibling).wait_recv()


def solution(mesh):
    dp, mp = mesh.shape["dp"], mesh.shape["mp"]

    def local(master, moment_first, moment_second, gradients, step_count, tensor_rows, decay_mask):
        rows, wide = master.shape
        tensors = tensor_rows.shape[0]
        chips = dp // 2
        full = pltpu.VMEM((rows, wide), jnp.float32)
        dma = pltpu.SemaphoreType.DMA
        hops = max(chips - 1, 1)
        return pl.pallas_call(
            functools.partial(kernel, dp, mp, tensors),
            out_shape=(full, full, full, pltpu.VMEM((dp * rows, wide), jnp.bfloat16)),
            in_specs=[pl.BlockSpec(memory_space=pltpu.SMEM)] * 3 + [pl.BlockSpec(memory_space=pltpu.HBM)] * 4,
            out_specs=(pl.BlockSpec(memory_space=pltpu.VMEM),) * 4,
            scratch_shapes=[
                full, full, full, full,
                pltpu.VMEM((1, 1, 128), jnp.float32),
                pltpu.VMEM((mp, 1, 128), jnp.float32),
                pltpu.VMEM((1, 1, 128), jnp.float32),
                pltpu.VMEM((dp, 1, 128), jnp.float32),
                dma((4, LOADS)), dma((mp,)), dma((mp,)), dma((dp,)), dma((dp,)),
                dma((hops, CHUNKS)), dma((hops, CHUNKS)), dma((hops, CHUNKS)), dma((hops, CHUNKS)),
                dma((chips, CHUNKS)), dma((chips, CHUNKS)),
            ],
            compiler_params=pltpu.CompilerParams(
                collective_id=0, has_side_effects=True, vmem_limit_bytes=20 * 1024 * 1024),
        )(step_count, tensor_rows, decay_mask, master, moment_first, moment_second, gradients)

    placed = (P("dp", "mp"), P("dp", "mp"), P("dp", "mp"), P("dp", "mp"), P(), P(), P())
    return jax.shard_map(
        local,
        mesh=mesh,
        in_specs=placed,
        out_specs=(P("dp", "mp"), P("dp", "mp"), P("dp", "mp"), P(None, "mp")),
        check_vma=False,
    )
```

```python
import functools

import jax
import jax.numpy as jnp
from jax import lax
from jax.experimental import pallas as pl
from jax.experimental.pallas import tpu as pltpu
from jax.sharding import PartitionSpec as P

MESH = pl.DeviceIdType.MESH

beta_first = 0.9
beta_second = 0.999
adam_epsilon = 1e-06
decay_rate = 0.3
learn_rate = 0.3
norm_epsilon = 1e-06

LOADS = 8
CHUNKS = 4
GROUP = 16
WRITES = 4
HALF = 64


def power(base, exponent):
    result = jnp.float32(1.0)
    factor = jnp.float32(base)
    for bit in range(31):
        taken = ((exponent >> bit) & 1) == 1
        result = jnp.where(taken, result * factor, result)
        factor = factor * factor
    return result


def kernel(dp, mp, tensors, step_ref, rows_hbm, mask_hbm, m_hbm, f_hbm, s_hbm, g_hbm,
           nm_ref, nf_ref, ns_ref, x_ref,
           mb, fb, sb, gb, mine, slots,
           rows_ref, mask_ref, small_sem, load_sem, sum_send, sum_recv,
           up_send, up_recv, down_send, down_recv, sib_send, sib_recv):
    rows, wide = m_hbm.shape
    me = lax.axis_index("dp")
    col = lax.axis_index("mp")
    chips = dp // 2
    chip, core = me // 2, me % 2
    sibling = me + 1 - 2 * core
    piece = rows // LOADS
    part = rows // CHUNKS

    def loads(i):
        at = pl.ds(i * piece, piece)
        pairs = ((m_hbm, mb), (f_hbm, fb), (s_hbm, sb), (g_hbm, gb))
        return [pltpu.make_async_copy(a.at[at], b.at[at], load_sem.at[n, i]) for n, (a, b) in enumerate(pairs)]

    pairs = ((rows_hbm, rows_ref), (mask_hbm, mask_ref))
    small = [pltpu.make_async_copy(a, b, small_sem.at[n]) for n, (a, b) in enumerate(pairs)]
    for copy in small:
        copy.start()
    for i in range(LOADS):
        for copy in loads(i):
            copy.start()

    count = dp * mp
    own = me * mp + col

    def peer(d):
        at = lax.rem(own + d, count)
        return {"dp": at // mp, "mp": lax.rem(at, mp)}

    barrier = pltpu.get_barrier_semaphore()

    def greet(d, carry):
        pl.semaphore_signal(barrier, inc=1, device_id=peer(d), device_id_type=MESH)
        return carry

    lax.fori_loop(1, count, greet, 0)

    for copy in small:
        copy.wait()
    step = step_ref[0]
    fix_first = 1.0 - power(beta_first, step)
    fix_second = 1.0 - power(beta_second, step)
    tile = (8, 128)
    scale = (jnp.full(tile, fix_first, jnp.float32) * lax.rsqrt(jnp.full(tile, fix_second, jnp.float32)))[0, 0]
    shift = fix_first * adam_epsilon

    lane = lax.broadcasted_iota(jnp.int32, (1, 128), 1)
    low = jnp.full((1, 128), -1, jnp.int32)
    high = jnp.full((1, 128), -1, jnp.int32)
    decay = jnp.zeros((1, 128), jnp.float32)
    offset = jnp.int32(0)
    for k in range(tensors):
        here = (lane == k) | (lane == HALF + k)
        after = offset + rows_ref[k]
        low = jnp.where(here, offset, low)
        high = jnp.where(here, after, high)
        decay = jnp.where(lane == k, decay_rate * mask_ref[k].astype(jnp.float32), decay)
        offset = after
    first_half = lane < HALF

    def member(start):
        ids = me * rows + start + lax.broadcasted_iota(jnp.int32, (GROUP, 128), 0)
        return ((ids >= low) & (ids < high)).astype(jnp.float32)

    def stats(i, total):
        at = pl.ds(pl.multiple_of(i * GROUP, GROUP), GROUP)
        inside = member(i * GROUP)
        decay_rows = jnp.sum(inside * decay, axis=1, keepdims=True)
        master, gradient = mb[at], gb[at]
        new_first = beta_first * fb[at] + (1.0 - beta_first) * gradient
        new_second = beta_second * sb[at] + (1.0 - beta_second) * gradient * gradient
        nf_ref[at] = new_first
        ns_ref[at] = new_second
        update = new_first / (scale * jnp.sqrt(new_second) + shift) + decay_rows * master
        gb[at] = update
        weight_sq = jnp.sum(master * master, axis=1, keepdims=True)
        update_sq = jnp.sum(update * update, axis=1, keepdims=True)
        return total + inside * jnp.where(first_half, weight_sq, update_sq)

    total = jnp.zeros((GROUP, 128), jnp.float32)
    steps = piece // GROUP
    for i in range(LOADS):
        for copy in loads(i):
            copy.wait()
        total = lax.fori_loop(i * steps, (i + 1) * steps, stats, total, unroll=True)
    total = jnp.sum(total, axis=0, keepdims=True)

    pl.semaphore_wait(barrier, count - 1)

    def share(d):
        return pltpu.make_async_remote_copy(
            src_ref=mine.at[0], dst_ref=slots.at[own], send_sem=sum_send.at[d], recv_sem=sum_recv.at[d],
            device_id=peer(d), device_id_type=MESH)

    def start_share(d, carry):
        share(d).start()
        return carry

    def wait_share(d, carry):
        share(d).wait_recv()
        return carry

    def sent_share(d, carry):
        share(d).wait_send()
        return carry

    mine[0] = total
    slots[own] = total
    lax.fori_loop(1, count, start_share, 0)
    lax.fori_loop(1, count, wait_share, 0)
    total = jnp.sum(slots[...], axis=0)
    root = jnp.sqrt(jnp.broadcast_to(total, tile))
    ratio = root / (pltpu.roll(root, HALF, 1) + norm_epsilon)
    ratio = jnp.where(first_half, learn_rate * ratio[0:1], 0.0)

    def block(owner, k):
        return x_ref.at[pl.ds(pl.multiple_of(owner * rows + k * part, part), part)]

    def up(s, k):
        ref = block(me - 2 * s, k)
        return pltpu.make_async_remote_copy(
            src_ref=ref, dst_ref=ref, send_sem=up_send.at[s, k], recv_sem=up_recv.at[s, k],
            device_id={"dp": me + 2}, device_id_type=MESH)

    def down(s, k):
        ref = block(me + 2 * s, k)
        return pltpu.make_async_remote_copy(
            src_ref=ref, dst_ref=ref, send_sem=down_send.at[s, k], recv_sem=down_recv.at[s, k],
            device_id={"dp": me - 2}, device_id_type=MESH)

    def side(j, k):
        ref = block(2 * j + core, k)
        return pltpu.make_async_remote_copy(
            src_ref=ref, dst_ref=ref, send_sem=sib_send.at[j, k], recv_sem=sib_recv.at[j, k],
            device_id={"dp": sibling}, device_id_type=MESH)

    def arrival(recv, s, owner, k, to):
        ref = block(owner, k)
        return pltpu.make_async_remote_copy(
            src_ref=ref, dst_ref=ref, send_sem=up_send.at[0, k], recv_sem=recv.at[s, k],
            device_id={"dp": to}, device_id_type=MESH)

    last = chips - 1

    def final(i, carry):
        at = pl.ds(pl.multiple_of(i * GROUP, GROUP), GROUP)
        rate = jnp.sum(member(i * GROUP) * ratio, axis=1, keepdims=True)
        new_master = mb[at] - rate * gb[at]
        nm_ref[at] = new_master
        x_ref[pl.ds(pl.multiple_of(me * rows + i * GROUP, GROUP), GROUP)] = new_master.astype(jnp.bfloat16)
        return carry

    def send_own(k):
        @pl.when(chip < last)
        def _():
            up(0, k).start()

        @pl.when(chip > 0)
        def _():
            down(0, k).start()

        side(chip, k).start()

    groups = part // GROUP
    for k in range(CHUNKS):
        lax.fori_loop(k * groups, (k + 1) * groups, final, 0, unroll=2)
        if k > 0:
            send_own(k - 1)
    lax.fori_loop(1, count, sent_share, 0)
    send_own(CHUNKS - 1)

    for s in range(last):
        for k in range(CHUNKS):
            @pl.when(s < chip)
            def _():
                arrival(up_recv, s, me - 2 * (s + 1), k, sibling).wait_recv()

                @pl.when(chip < last)
                def _():
                    up(s + 1, k).start()

                side(chip - (s + 1), k).start()

            @pl.when(s < last - chip)
            def _():
                arrival(down_recv, s, me + 2 * (s + 1), k, sibling).wait_recv()

                @pl.when(chip > 0)
                def _():
                    down(s + 1, k).start()

                side(chip + (s + 1), k).start()

    for s in range(chips):
        for k in range(CHUNKS):
            if s < last or last == 0:
                @pl.when((chip < last) & (s <= chip))
                def _():
                    up(s, k).wait_send()

                @pl.when((chip > 0) & (s <= last - chip))
                def _():
                    down(s, k).wait_send()

            side(s, k).wait_send()
            arrival(sib_recv, s, 2 * s + 1 - core, k, sibling).wait_recv()


def flush(*refs):
    count = (len(refs) - 1) // 2
    sems = refs[-1]
    copies = []
    for n, (source, target) in enumerate(zip(refs[:count], refs[count:2 * count])):
        piece = source.shape[0] // WRITES
        for i in range(WRITES):
            at = pl.ds(i * piece, piece)
            copies.append(pltpu.make_async_copy(source.at[at], target.at[at], sems.at[n, i]))
    for copy in copies:
        copy.start()
    for copy in copies:
        copy.wait()


def solution(mesh):
    dp, mp = mesh.shape["dp"], mesh.shape["mp"]

    def local(master, moment_first, moment_second, gradients, step_count, tensor_rows, decay_mask):
        rows, wide = master.shape
        tensors = tensor_rows.shape[0]
        chips = dp // 2
        full = pltpu.VMEM((rows, wide), jnp.float32)
        dma = pltpu.SemaphoreType.DMA
        hops = max(chips - 1, 1)
        operands = (tensor_rows, decay_mask, master, moment_first, moment_second, gradients)
        operands = [pltpu.with_memory_space_constraint(a, pltpu.HBM) for a in operands]
        held = pl.pallas_call(
            functools.partial(kernel, dp, mp, tensors),
            out_shape=(full, full, full, pltpu.VMEM((dp * rows, wide), jnp.bfloat16)),
            in_specs=[pl.BlockSpec(memory_space=pltpu.SMEM)] + [pl.BlockSpec(memory_space=pltpu.HBM)] * 6,
            out_specs=(pl.BlockSpec(memory_space=pltpu.VMEM),) * 4,
            scratch_shapes=[
                full, full, full, full,
                pltpu.VMEM((1, 1, 128), jnp.float32),
                pltpu.VMEM((dp * mp, 1, 128), jnp.float32),
                pltpu.SMEM(tensor_rows.shape, jnp.int32),
                pltpu.SMEM(decay_mask.shape, jnp.int32), dma((2,)),
                dma((4, LOADS)), dma((dp * mp,)), dma((dp * mp,)),
                dma((hops, CHUNKS)), dma((hops, CHUNKS)), dma((hops, CHUNKS)), dma((hops, CHUNKS)),
                dma((chips, CHUNKS)), dma((chips, CHUNKS)),
            ],
            compiler_params=pltpu.CompilerParams(
                collective_id=0, has_side_effects=True, vmem_limit_bytes=20 * 1024 * 1024),
        )(step_count, *operands)
        return pl.pallas_call(
            flush,
            out_shape=tuple(jax.ShapeDtypeStruct(a.shape, a.dtype) for a in held),
            in_specs=[pl.BlockSpec(memory_space=pltpu.VMEM)] * 4,
            out_specs=(pl.BlockSpec(memory_space=pltpu.HBM),) * 4,
            scratch_shapes=[dma((4, WRITES))],
            compiler_params=pltpu.CompilerParams(vmem_limit_bytes=1024 * 1024),
        )(*held)

    placed = (P("dp", "mp"), P("dp", "mp"), P("dp", "mp"), P("dp", "mp"), P(), P(), P())
    return jax.shard_map(
        local,
        mesh=mesh,
        in_specs=placed,
        out_specs=(P("dp", "mp"), P("dp", "mp"), P("dp", "mp"), P(None, "mp")),
        check_vma=False,
    )
```
